16 devices in a mesh: dp: 2 (over y, z), ctx: 8 (over x, core).
Axes of the slice: x: 4, y: 2, z: 1, core: 2. Of those that a mesh axis runs over, the one named last changes fastest.
The devices are a block of a 4x4x8 slice.
Arguments:
- q_seq: bfloat16 [2, 8192, 8, 256], P('dp', 'ctx'), parts along dimension 0
- k_seq: bfloat16 [2, 8192, 4, 256], P('dp', 'ctx'), parts along dimension 0
- v_seq: bfloat16 [2, 8192, 4, 256], P('dp', 'ctx'), parts along dimension 0
- do_seq: bfloat16 [2, 8192, 8, 256], P('dp', 'ctx'), parts along dimension 0
Outputs:
- output 1: bfloat16 [2, 8192, 8, 256], P('dp', 'ctx'), parts along dimension 0
- output 2: bfloat16 [2, 8192, 8, 256], P('dp', 'ctx'), parts along dimension 0
- output 3: bfloat16 [2, 8192, 4, 256], P('dp', 'ctx'), parts along dimension 0
- output 4: bfloat16 [2, 8192, 4, 256], P('dp', 'ctx'), parts along dimension 0
There are 2 independent parts. The reference program is written for one: setup_inputs(seed, part) draws one part's arguments, and reference() takes and returns one part's arrays. A program takes and returns all parts, laid end to end along the dimension named above; each array names one.
All inputs are finite; a program needn't handle non-finite values.
Results may differ from the reference program's by a relative error of at most 0.00872058.
Values are sent between devices in bfloat16 or wider.
A program may use at most 768 MiB of HBM per device.

```python
import math
import jax
import jax.numpy as jnp
from jax import lax

BATCH = 1
CTX = 8
CHUNK = 1024
Q_HEADS = 8
KV_LOCAL = 4
HEAD = 256
WINDOW = 4096

SEQ = CTX * CHUNK
GROUP = Q_HEADS // KV_LOCAL
QBLK = min(CHUNK, 128)
NEG_BIG = -1e30


def setup_inputs(seed: int = 0, part: int = 0) -> dict:
    base_key = jax.random.fold_in(jax.random.key(seed), part)
    key_q, key_k, key_v, key_do = jax.random.split(base_key, 4)
    input_std = (0.5 * math.log(WINDOW)) ** 0.25
    q_shape = (BATCH, SEQ, Q_HEADS, HEAD)
    kv_shape = (BATCH, SEQ, KV_LOCAL, HEAD)
    q_seq = input_std * jax.random.normal(key_q, q_shape, jnp.float32)
    k_seq = input_std * jax.random.normal(key_k, kv_shape, jnp.float32)
    v_seq = jax.random.normal(key_v, kv_shape, jnp.float32)
    do_seq = jax.random.normal(key_do, q_shape, jnp.float32)
    return {'q_seq': q_seq.astype(jnp.bfloat16), 'k_seq': k_seq.astype(jnp.bfloat16), 'v_seq': v_seq.astype(jnp.bfloat16), 'do_seq': do_seq.astype(jnp.bfloat16)}


def attend_all(q_full, k_full, v_full):
    n_blk = SEQ // QBLK
    q_blocks = jnp.moveaxis(q_full.reshape(BATCH, n_blk, QBLK, KV_LOCAL, GROUP, HEAD), 1, 0)
    pad_width = ((0, 0), (WINDOW, 0), (0, 0), (0, 0))
    k_pad = jnp.pad(k_full, pad_width)
    v_pad = jnp.pad(v_full, pad_width)
    span_len = WINDOW + QBLK
    dist = jnp.arange(QBLK)[:, None] + WINDOW - jnp.arange(span_len)[None, :]
    pair_ok = (dist >= 0) & (dist < WINDOW)
    sm_scale = HEAD ** -0.5

    def one_block(blk_args):
        blk_id, q_blk = blk_args
        start = blk_id * QBLK
        k_win = lax.dynamic_slice_in_dim(k_pad, start, span_len, axis=1)
        v_win = lax.dynamic_slice_in_dim(v_pad, start, span_len, axis=1)
        keep_mask = pair_ok & (jnp.arange(span_len)[None, :] + start >= WINDOW)
        scores = jnp.einsum('bqhgd,bkhd->bhgqk', q_blk, k_win) * sm_scale
        scores = jnp.where(keep_mask, scores, NEG_BIG)
        weights = jax.nn.softmax(scores, axis=-1)
        return jnp.einsum('bhgqk,bkhd->bqhgd', weights, v_win)

    o_blocks = lax.map(jax.checkpoint(one_block), (jnp.arange(n_blk), q_blocks))
    return jnp.moveaxis(o_blocks, 0, 1).reshape(BATCH, SEQ, Q_HEADS, HEAD)


def reference(q_seq, k_seq, v_seq, do_seq):
    o_full, pull_back = jax.vjp(attend_all, q_seq.astype(jnp.float32), k_seq.astype(jnp.float32), v_seq.astype(jnp.float32))
    dq_full, dk_full, dv_full = pull_back(do_seq.astype(jnp.float32))
    return (o_full.astype(jnp.bfloat16), dq_full.astype(jnp.bfloat16), dk_full.astype(jnp.bfloat16), dv_full.astype(jnp.bfloat16))
```

```python
import functools
import math

import jax
import jax.numpy as jnp
from jax import lax
from jax.experimental import pallas as pl
from jax.experimental.pallas import tpu as pltpu
from jax.sharding import PartitionSpec as P

WINDOW = 4096
NEG_BIG = -1e30
BLK = 512


def dot_nn(a, b):
    return lax.dot_general(a, b, (((1,), (0,)), ((), ())), preferred_element_type=jnp.float32)


def dot_nt(a, b):
    return lax.dot_general(a, b, (((1,), (1,)), ((), ())), preferred_element_type=jnp.float32)


def attn_kernel(q_ref, do_ref, k_ref, v_ref, o_ref, dq_ref, dk_ref, dv_ref, kt_ref, acc_ref, m_ref, l_ref, lse_ref, dqt_ref):
    n_chip, n_grp, chunk, dim = q_ref.shape
    core = lax.rem(lax.axis_index('ctx'), 2)
    per = chunk // BLK
    win = WINDOW // BLK
    scale = dim ** -0.5
    coef = scale * math.log2(math.e)

    def kv_slot(kb):
        chk = kb // per
        side = lax.rem(chk + core, 2)
        rows = pl.ds(pl.multiple_of(lax.rem(kb, per) * BLK, BLK), BLK)
        return side, chk // 2, rows

    def two_heads(ref, m, rows):
        return jnp.concatenate([ref[m, h, rows, :] for h in range(n_grp)], axis=0)

    for side in range(2):
        def tr_body(m, carry):
            kt_ref[side, m] = jnp.transpose(k_ref[side, m])
            return carry
        lax.fori_loop(0, n_chip, tr_body, 0)

    def zero_body(m, carry):
        for side in range(2):
            dk_ref[side, m] = jnp.zeros((chunk, dim), jnp.float32)
            dv_ref[side, m] = jnp.zeros((chunk, dim), jnp.float32)
        return carry
    lax.fori_loop(0, n_chip, zero_body, 0)

    tok_q = lax.rem(lax.broadcasted_iota(jnp.int32, (n_grp * BLK, BLK), 0), BLK)
    tok_k = lax.broadcasted_iota(jnp.int32, (n_grp * BLK, BLK), 1)
    tok_qt = lax.rem(lax.broadcasted_iota(jnp.int32, (BLK, n_grp * BLK), 1), BLK)
    tok_kt = lax.broadcasted_iota(jnp.int32, (BLK, n_grp * BLK), 0)

    def q_body(step, carry):
        m = step // per
        t = lax.rem(step, per)
        rows = pl.ds(pl.multiple_of(t * BLK, BLK), BLK)
        blk = (2 * m + core) * per + t
        lo = jnp.maximum(blk - win + 1, 0)

        def fwd(kb, kind):
            side, mk, krows = kv_slot(kb)
            s = dot_nt(two_heads(q_ref, m, rows), k_ref[side, mk, krows, :])
            if kind == 'diag':
                s = jnp.where(tok_k <= tok_q, s, NEG_BIG)
            elif kind == 'far':
                s = jnp.where(tok_k > tok_q, s, NEG_BIG)
            s_max = jnp.max(s, axis=1, keepdims=True)
            if kind == 'diag':
                m_new = jnp.broadcast_to(s_max, (n_grp * BLK, 128))
            else:
                m_old = m_ref[...]
                m_new = jnp.maximum(m_old, s_max)
                alpha = jnp.exp2((m_old - m_new) * coef)
            p = jnp.exp2(s * coef - (m_new * coef)[:, :1])
            p_sum = jnp.sum(p, axis=1, keepdims=True)
            pv = dot_nn(p.astype(jnp.bfloat16), v_ref[side, mk, krows, :])
            m_ref[...] = m_new
            if kind == 'diag':
                l_ref[...] = jnp.broadcast_to(p_sum, (n_grp * BLK, 128))
                acc_ref[...] = pv
            else:
                l_ref[...] = l_ref[...] * alpha + p_sum
                acc_ref[...] = acc_ref[...] * alpha[:, :1] + pv

        fwd(blk, 'diag')
        lax.fori_loop(lo, blk, lambda kb, c: (fwd(kb, 'full'), c)[1], 0)
        pl.when(blk >= win)(lambda: fwd(blk - win, 'far'))

        l_tot = l_ref[...]
        o = (acc_ref[...] * (1.0 / l_tot)[:, :1]).astype(jnp.bfloat16)
        for h in range(n_grp):
            o_ref[m, h, rows, :] = o[h * BLK:(h + 1) * BLK]
        lse_ref[0:1, :] = jnp.transpose(m_ref[...] * coef + jnp.log2(l_tot))[0:1, :]
        drow = jnp.sum(two_heads(do_ref, m, rows).astype(jnp.float32) * o.astype(jnp.float32), axis=1, keepdims=True)
        lse_ref[1:2, :] = jnp.transpose(jnp.broadcast_to(drow, (n_grp * BLK, 128)))[0:1, :]

        def bwd(kb, kind):
            side, mk, krows = kv_slot(kb)
            q2 = two_heads(q_ref, m, rows)
            do2 = two_heads(do_ref, m, rows)
            st = dot_nt(k_ref[side, mk, krows, :], q2)
            if kind == 'diag':
                st = jnp.where(tok_kt <= tok_qt, st, NEG_BIG)
            elif kind == 'far':
                st = jnp.where(tok_kt > tok_qt, st, NEG_BIG)
            dpt = dot_nt(v_ref[side, mk, krows, :], do2)
            p = jnp.exp2(st * coef - lse_ref[0:1, :])
            ds = (p * (dpt - lse_ref[1:2, :])).astype(jnp.bfloat16)
            dv_ref[side, mk, krows, :] += dot_nn(p.astype(jnp.bfloat16), do2)
            dk_ref[side, mk, krows, :] += dot_nn(ds, q2)
            dqt = dot_nn(kt_ref[side, mk, :, krows], ds)
            if kind == 'diag':
                dqt_ref[...] = dqt
            else:
                dqt_ref[...] += dqt

        bwd(blk, 'diag')
        lax.fori_loop(lo, blk, lambda kb, c: (bwd(kb, 'full'), c)[1], 0)
        pl.when(blk >= win)(lambda: bwd(blk - win, 'far'))
        dq = jnp.transpose(dqt_ref[...] * scale).astype(jnp.bfloat16)
        for h in range(n_grp):
            dq_ref[m, h, rows, :] = dq[h * BLK:(h + 1) * BLK]
        return carry

    lax.fori_loop(0, n_chip * per, q_body, 0)

    def scale_body(m, carry):
        for side in range(2):
            dk_ref[side, m] *= scale
        return carry
    lax.fori_loop(0, n_chip, scale_body, 0)


def solution(mesh):
    n_ctx = mesh.shape['ctx']
    n_chip = n_ctx // 2
    seq_spec = P('dp', 'ctx', None, None)
    groups = [[2 * x + c for x in range(n_chip)] for c in range(2)]
    swap = [(j, j ^ 1) for j in range(n_ctx)]

    def a2a(x):
        return lax.all_to_all(x, 'ctx', 0, 0, axis_index_groups=groups, tiled=True)

    def local_attn(q_loc, k_loc, v_loc, do_loc):
        _, chunk, q_heads, dim = q_loc.shape
        kv_heads = k_loc.shape[2]
        n_grp = q_heads // kv_heads

        def spread_q(x):
            return a2a(jnp.transpose(x.reshape(chunk, kv_heads, n_grp, dim), (1, 2, 0, 3)))

        def spread_kv(x):
            own = a2a(jnp.transpose(x.reshape(chunk, kv_heads, dim), (1, 0, 2)))
            return jnp.stack([own, lax.ppermute(own, 'ctx', swap)])

        k_all, v_all, q_all, do_all = spread_kv(k_loc), spread_kv(v_loc), spread_q(q_loc), spread_q(do_loc)
        q_type = jax.ShapeDtypeStruct((n_chip, n_grp, chunk, dim), jnp.bfloat16)
        kv_type = jax.ShapeDtypeStruct((2, n_chip, chunk, dim), jnp.float32)
        rows = n_grp * BLK
        o_all, dq_all, dk_all, dv_all = pl.pallas_call(
            attn_kernel,
            out_shape=(q_type, q_type, kv_type, kv_type),
            in_specs=[pl.BlockSpec(memory_space=pltpu.VMEM)] * 4,
            out_specs=[pl.BlockSpec(memory_space=pltpu.VMEM)] * 4,
            scratch_shapes=[
                pltpu.VMEM((2, n_chip, dim, chunk), jnp.bfloat16),
                pltpu.VMEM((rows, dim), jnp.float32),
                pltpu.VMEM((rows, 128), jnp.float32),
                pltpu.VMEM((rows, 128), jnp.float32),
                pltpu.VMEM((8, rows), jnp.float32),
                pltpu.VMEM((dim, rows), jnp.float32),
            ],
            compiler_params=pltpu.CompilerParams(vmem_limit_bytes=64000 * 1024),
        )(q_all, do_all, k_all, v_all)

        def home_q(x):
            return jnp.transpose(a2a(x), (2, 0, 1, 3)).reshape(q_loc.shape)

        def home_kv(x):
            total = (x[0] + lax.ppermute(x[1], 'ctx', swap)).astype(jnp.bfloat16)
            return jnp.transpose(a2a(total), (1, 0, 2)).reshape(k_loc.shape)

        return home_q(o_all), home_q(dq_all), home_kv(dk_all), home_kv(dv_all)

    return jax.shard_map(local_attn, mesh=mesh, in_specs=(seq_spec,) * 4, out_specs=(seq_spec,) * 4, check_vma=False)
```

```python
import math

import jax
import jax.numpy as jnp
from jax import lax
from jax.experimental import pallas as pl
from jax.experimental.pallas import tpu as pltpu
from jax.sharding import PartitionSpec as P

WINDOW = 4096
NEG_BIG = -1e30
MESH = pl.DeviceIdType.MESH
K, V, KX, VX, Q, DO, O, DQ, DK, DV, DKX, DVX = range(12)


def dot_nn(a, b):
    return lax.dot_general(a, b, (((1,), (0,)), ((), ())), preferred_element_type=jnp.float32)


def dot_nt(a, b):
    return lax.dot_general(a, b, (((1,), (1,)), ((), ())), preferred_element_type=jnp.float32)


def attn_kernel(q_in, do_in, k_in, v_in, o_out, dq_out, dk_out, dv_out,
                q_all, do_all, k_all, v_all, kt_all, dk_all, dv_all, o_all, dq_all, dkx, dvx,
                acc_ref, m_ref, l_ref, lse_ref, dqt_ref, send_sem, recv_sem):
    n_chip, n_half, n_grp, blk_len, dim = q_in.shape
    chunk = n_half * blk_len
    n_dev = 2 * n_chip
    rows2 = n_grp * blk_len
    me = lax.axis_index('ctx')
    chip, core = me // 2, lax.rem(me, 2)
    win = WINDOW // blk_len
    scale = dim ** -0.5
    coef = scale * math.log2(math.e)

    def order(i):
        return i + i // 2 - 2 * (i // 3)

    def ahead(s):
        return lax.rem(chip + s, n_chip)

    def behind(s):
        return lax.rem(chip + n_chip - s, n_chip)

    def remote(kind, idx, src, dst, to_chip, to_core):
        return pltpu.make_async_remote_copy(
            src_ref=src, dst_ref=dst, send_sem=send_sem.at[kind, idx], recv_sem=recv_sem.at[kind, idx],
            device_id={'ctx': 2 * to_chip + to_core}, device_id_type=MESH)

    def local(kind, idx, src, dst):
        return pltpu.make_async_copy(src, dst, recv_sem.at[kind, idx])

    barrier = pltpu.get_barrier_semaphore()
    for step in range(1, n_dev):
        pl.semaphore_signal(barrier, inc=1, device_id={'ctx': lax.rem(me + step, n_dev)}, device_id_type=MESH)
    pl.semaphore_wait(barrier, n_dev - 1)

    def send_kv(kind, s):
        src, dst = ((k_in, k_all), (v_in, v_all))[kind]
        return remote(kind, s, src.at[ahead(s)], dst.at[0, chip], ahead(s), core)

    def send_q(kind, s, t):
        src, dst = ((q_in, q_all), (do_in, do_all))[kind - Q]
        return remote(kind, 2 * s + t, src.at[ahead(s), t], dst.at[chip, t], ahead(s), lax.rem(core + t, 2))

    own_copies = (local(K, 0, k_in.at[chip], k_all.at[0, chip]), local(V, 0, v_in.at[chip], v_all.at[0, chip]),
                  local(Q, 0, q_in.at[chip, 0], q_all.at[chip, 0]), local(DO, 0, do_in.at[chip, 0], do_all.at[chip, 0]))
    sends = []
    for s in (1, 3, 2):
        sends += [send_kv(K, s), send_kv(V, s)]
    for pair in ((1, 3), (2,)):
        for kind in (Q, DO):
            sends += [send_q(kind, s, t) for s in pair for t in range(2)]
    sends += [send_q(Q, 0, 1), send_q(DO, 0, 1)]
    for copy in own_copies:
        copy.start()
    for copy in sends:
        copy.start()

    def zero_body(m, carry):
        for side in range(2):
            dk_all[side, m] = jnp.zeros((chunk, dim), jnp.float32)
            dv_all[side, m] = jnp.zeros((chunk, dim), jnp.float32)
        return carry
    lax.fori_loop(0, n_chip, zero_body, 0)

    def pass_on(kind, s):
        ref = (k_all, v_all)[kind - KX]
        return remote(kind, s, ref.at[0, behind(s)], ref.at[1, behind(s)], chip, 1 - core)

    def own_side(i, carry):
        s = order(i)
        m = behind(s)

        @pl.when(i == 0)
        def _():
            own_copies[0].wait()
            own_copies[1].wait()

        @pl.when(i > 0)
        def _():
            remote(K, s, k_in.at[0], k_all.at[0, m], chip, core).wait_recv()
            remote(V, s, v_in.at[0], v_all.at[0, m], chip, core).wait_recv()
        pass_on(KX, s).start()
        pass_on(VX, s).start()
        kt_all[0, m] = jnp.transpose(k_all[0, m])
        return carry
    lax.fori_loop(0, n_chip, own_side, 0)

    def other_side(i, carry):
        s = order(i)
        m = behind(s)
        pass_on(KX, s).wait_recv()
        pass_on(VX, s).wait_recv()
        kt_all[1, m] = jnp.transpose(k_all[1, m])
        return carry
    lax.fori_loop(0, n_chip, other_side, 0)

    def kv_slot(kb):
        chk = kb // n_half
        rows = pl.ds(pl.multiple_of(lax.rem(kb, n_half) * blk_len, blk_len), blk_len)
        return lax.rem(chk + core, 2), chk // 2, rows

    tok_q = lax.rem(lax.broadcasted_iota(jnp.int32, (rows2, blk_len), 0), blk_len)
    tok_k = lax.broadcasted_iota(jnp.int32, (rows2, blk_len), 1)
    tok_qt = lax.rem(lax.broadcasted_iota(jnp.int32, (blk_len, rows2), 1), blk_len)
    tok_kt = lax.broadcasted_iota(jnp.int32, (blk_len, rows2), 0)

    def q_body(step, carry):
        s = order(lax.rem(step // 2 + 1, n_chip))
        u = lax.rem(step, 2)
        m = behind(s)
        idx = 2 * s + u
        is_own = step == 2 * n_chip - 2

        @pl.when(is_own)
        def _():
            own_copies[2].wait()
            own_copies[3].wait()

        @pl.when(jnp.logical_not(is_own))
        def _():
            remote(Q, idx, q_in.at[0, 0], q_all.at[m, u], chip, core).wait_recv()
            remote(DO, idx, do_in.at[0, 0], do_all.at[m, u], chip, core).wait_recv()

        blk = 2 * n_half * m + 2 * core + u * (3 - 4 * core)
        lo = jnp.maximum(blk - win + 1, 0)

        def fwd(kb, kind):
            side, mk, krows = kv_slot(kb)
            sc = dot_nt(q_all[m, u].reshape(rows2, dim), k_all[side, mk, krows, :])
            if kind == 'diag':
                sc = jnp.where(tok_k <= tok_q, sc, NEG_BIG)
            elif kind == 'far':
                sc = jnp.where(tok_k > tok_q, sc, NEG_BIG)
            s_max = jnp.max(sc, axis=1, keepdims=True)
            if kind == 'diag':
                m_new = jnp.broadcast_to(s_max, (rows2, 128))
            else:
                m_old = m_ref[...]
                m_new = jnp.maximum(m_old, s_max)
                alpha = jnp.exp2((m_old - m_new) * coef)
            p = jnp.exp2(sc * coef - (m_new * coef)[:, :1])
            p_sum = jnp.sum(p, axis=1, keepdims=True)
            pv = dot_nn(p.astype(jnp.bfloat16), v_all[side, mk, krows, :])
            m_ref[...] = m_new
            if kind == 'diag':
                l_ref[...] = jnp.broadcast_to(p_sum, (rows2, 128))
                acc_ref[...] = pv
            else:
                l_ref[...] = l_ref[...] * alpha + p_sum
                acc_ref[...] = acc_ref[...] * alpha[:, :1] + pv

        fwd(blk, 'diag')
        lax.fori_loop(lo, blk, lambda kb, c: (fwd(kb, 'full'), c)[1], 0)
        pl.when(blk >= win)(lambda: fwd(blk - win, 'far'))

        l_tot = l_ref[...]
        o = (acc_ref[...] * (1.0 / l_tot)[:, :1]).astype(jnp.bfloat16)
        o_all[m, u] = o.reshape(n_grp, blk_len, dim)
        lse_ref[0:1, :] = jnp.transpose(m_ref[...] * coef + jnp.log2(l_tot))[0:1, :]
        drow = jnp.sum(do_all[m, u].reshape(rows2, dim).astype(jnp.float32) * o.astype(jnp.float32), axis=1, keepdims=True)
        lse_ref[1:2, :] = jnp.transpose(jnp.broadcast_to(drow, (rows2, 128)))[0:1, :]

        @pl.when(is_own)
        def _():
            local(O, 0, o_all.at[chip, 0], o_out.at[chip, 0]).start()

        @pl.when(jnp.logical_not(is_own))
        def _():
            remote(O, idx, o_all.at[m, u], o_out.at[chip, u], m, lax.rem(core + u, 2)).start()

        def bwd(kb, kind):
            side, mk, krows = kv_slot(kb)
            q2 = q_all[m, u].reshape(rows2, dim)
            do2 = do_all[m, u].reshape(rows2, dim)
            st = dot_nt(k_all[side, mk, krows, :], q2)
            if kind == 'diag':
                st = jnp.where(tok_kt <= tok_qt, st, NEG_BIG)
            elif kind == 'far':
                st = jnp.where(tok_kt > tok_qt, st, NEG_BIG)
            dpt = dot_nt(v_all[side, mk, krows, :], do2)
            p = jnp.exp2(st * coef - lse_ref[0:1, :])
            ds = (p * (dpt - lse_ref[1:2, :])).astype(jnp.bfloat16)
            dv_all[side, mk, krows, :] += dot_nn(p.astype(jnp.bfloat16), do2)
            dk_all[side, mk, krows, :] += dot_nn(ds, q2)
            dqt = dot_nn(kt_all[side, mk, :, krows], ds)
            if kind == 'diag':
                dqt_ref[...] = dqt
            else:
                dqt_ref[...] += dqt

        bwd(blk, 'diag')
        lax.fori_loop(lo, blk, lambda kb, c: (bwd(kb, 'full'), c)[1], 0)
        pl.when(blk >= win)(lambda: bwd(blk - win, 'far'))
        dq_all[m, u] = jnp.transpose(dqt_ref[...] * scale).astype(jnp.bfloat16).reshape(n_grp, blk_len, dim)

        @pl.when(is_own)
        def _():
            local(DQ, 0, dq_all.at[chip, 0], dq_out.at[chip, 0]).start()

        @pl.when(jnp.logical_not(is_own))
        def _():
            remote(DQ, idx, dq_all.at[m, u], dq_out.at[chip, u], m, lax.rem(core + u, 2)).start()
        return carry

    lax.fori_loop(0, 2 * n_chip, q_body, 0)

    def swap(kind, m):
        src, dst = ((dk_all, dkx), (dv_all, dvx))[kind - DKX]
        return remote(kind, m, src.at[1, m], dst.at[m], chip, 1 - core)

    def swap_body(i, carry):
        m = behind(order(lax.rem(i + 1, n_chip)))
        swap(DKX, m).start()
        swap(DVX, m).start()
        return carry
    lax.fori_loop(0, n_chip, swap_body, 0)

    for i in range(n_chip):
        s = (i + 1) + (i + 1) // 2 - 2 * ((i + 1) // 3) if i < n_chip - 1 else 0
        m = behind(s)
        pass_on(KX, s).wait_send()
        pass_on(VX, s).wait_send()
        for kind, part, other, buf, out, mul in ((DK, dk_all, dkx, k_all, dk_out, scale), (DV, dv_all, dvx, v_all, dv_out, 1.0)):
            swap(kind + 2, m).wait_recv()

            def add_body(r, carry):
                rows = pl.ds(pl.multiple_of(r * 256, 256), 256)
                buf[0, m, rows, :] = ((part[0, m, rows, :] + other[m, rows, :]) * mul).astype(jnp.bfloat16)
                return carry
            lax.fori_loop(0, chunk // 256, add_body, 0)
            if s == 0:
                local(kind, 0, buf.at[0, chip], out.at[chip]).start()
            else:
                remote(kind, s, buf.at[0, m], out.at[chip], m, core).start()

    for copy in sends:
        copy.wait_send()
    for s in range(n_chip):
        m = behind(s)
        h = ahead(s)
        swap(DKX, m).wait_send()
        swap(DVX, m).wait_send()
        for kind, buf, out in ((O, o_all, o_out), (DQ, dq_all, dq_out)):
            for t in range(2):
                if s == 0 and t == 0:
                    local(kind, 0, buf.at[chip, 0], out.at[chip, 0]).wait()
                else:
                    remote(kind, 2 * s + t, buf.at[m, t], out.at[chip, t], m, lax.rem(core + t, 2)).wait_send()
                    remote(kind, 2 * s + t, buf.at[m, t], out.at[h, t], m, core).wait_recv()
        for kind, buf, out in ((DK, k_all, dk_out), (DV, v_all, dv_out)):
            if s == 0:
                local(kind, 0, buf.at[0, chip], out.at[chip]).wait()
            else:
                remote(kind, s, buf.at[0, m], out.at[chip], m, core).wait_send()
                remote(kind, s, buf.at[0, m], out.at[h], m, core).wait_recv()


def solution(mesh):
    n_chip = mesh.shape['ctx'] // 2
    seq_spec = P('dp', 'ctx', None, None)

    def local_attn(q_loc, k_loc, v_loc, do_loc):
        _, chunk, q_heads, dim = q_loc.shape
        kv_heads = k_loc.shape[2]
        n_grp = q_heads // kv_heads
        blk_len = chunk // 2
        rows = n_grp * blk_len
        bf16, f32 = jnp.bfloat16, jnp.float32

        def split_q(x):
            return jnp.transpose(x.reshape(2, blk_len, kv_heads, n_grp, dim), (2, 0, 3, 1, 4))

        def split_kv(x):
            return jnp.transpose(x.reshape(chunk, kv_heads, dim), (1, 0, 2))

        q_shape, kv_shape = (n_chip, 2, n_grp, blk_len, dim), (n_chip, chunk, dim)
        q_type, kv_type = jax.ShapeDtypeStruct(q_shape, bf16), jax.ShapeDtypeStruct(kv_shape, bf16)
        o_all, dq_all, dk_all, dv_all = pl.pallas_call(
            attn_kernel,
            out_shape=(q_type, q_type, kv_type, kv_type),
            in_specs=[pl.BlockSpec(memory_space=pl.ANY)] * 4,
            out_specs=[pl.BlockSpec(memory_space=pl.ANY)] * 4,
            scratch_shapes=[
                pltpu.VMEM(q_shape, bf16),
                pltpu.VMEM(q_shape, bf16),
                pltpu.VMEM((2,) + kv_shape, bf16),
                pltpu.VMEM((2,) + kv_shape, bf16),
                pltpu.VMEM((2, n_chip, dim, chunk), bf16),
                pltpu.VMEM((2,) + kv_shape, f32),
                pltpu.VMEM((2,) + kv_shape, f32),
                pltpu.VMEM(q_shape, bf16),
                pltpu.VMEM(q_shape, bf16),
                pltpu.VMEM(kv_shape, f32),
                pltpu.VMEM(kv_shape, f32),
                pltpu.VMEM((rows, dim), f32),
                pltpu.VMEM((rows, 128), f32),
                pltpu.VMEM((rows, 128), f32),
                pltpu.VMEM((8, rows), f32),
                pltpu.VMEM((dim, rows), f32),
                pltpu.SemaphoreType.DMA((12, 8)),
                pltpu.SemaphoreType.DMA((12, 8)),
            ],
            compiler_params=pltpu.CompilerParams(vmem_limit_bytes=67043328, collective_id=0, has_side_effects=True),
        )(split_q(q_loc), split_q(do_loc), split_kv(k_loc), split_kv(v_loc))

        def join_q(x):
            return jnp.transpose(x, (1, 3, 0, 2, 4)).reshape(q_loc.shape)

        def join_kv(x):
            return jnp.transpose(x, (1, 0, 2)).reshape(k_loc.shape)

        return join_q(o_all), join_q(dq_all), join_kv(dk_all), join_kv(dv_all)

    return jax.shard_map(local_attn, mesh=mesh, in_specs=(seq_spec,) * 4, out_specs=(seq_spec,) * 4, check_vma=False)
```

```python
import math

import jax
import jax.numpy as jnp
from jax import lax
from jax.experimental import pallas as pl
from jax.experimental.pallas import tpu as pltpu
from jax.sharding import PartitionSpec as P

WINDOW = 4096
NEG_BIG = -1e30
MESH = pl.DeviceIdType.MESH
K, V, KX, VX, Q, DO, O, DQ, DK, DV, DKX, DVX = range(12)


def dot_nn(a, b):
    return lax.dot_general(a, b, (((1,), (0,)), ((), ())), preferred_element_type=jnp.float32)


def dot_nt(a, b):
    return lax.dot_general(a, b, (((1,), (1,)), ((), ())), preferred_element_type=jnp.float32)


def attn_kernel(q_in, do_in, k_in, v_in, o_out, dq_out, dk_out, dv_out,
                q_all, do_all, k_all, v_all, kt_all, dk_all, dv_all, o_all, dq_all, dkx, dvx,
                acc_ref, m_ref, l_ref, stat_ref, dqt_ref, send_sem, recv_sem):
    n_chip, n_half, n_grp, blk_len, dim = q_in.shape
    chunk = n_half * blk_len
    n_dev = 2 * n_chip
    rows2 = n_grp * blk_len
    me = lax.axis_index('ctx')
    chip, core = me // 2, lax.rem(me, 2)
    win = WINDOW // blk_len
    scale = dim ** -0.5
    coef = scale * math.log2(math.e)

    def order(i):
        return i + i // 2 - 2 * (i // 3)

    def ahead(s):
        return lax.rem(chip + s, n_chip)

    def behind(s):
        return lax.rem(chip + n_chip - s, n_chip)

    def remote(kind, idx, src, dst, to_chip, to_core):
        return pltpu.make_async_remote_copy(
            src_ref=src, dst_ref=dst, send_sem=send_sem.at[kind, idx], recv_sem=recv_sem.at[kind, idx],
            device_id={'ctx': 2 * to_chip + to_core}, device_id_type=MESH)

    def local(kind, idx, src, dst):
        return pltpu.make_async_copy(src, dst, recv_sem.at[kind, idx])

    barrier = pltpu.get_barrier_semaphore()
    for step in range(1, n_dev):
        pl.semaphore_signal(barrier, inc=1, device_id={'ctx': lax.rem(me + step, n_dev)}, device_id_type=MESH)
    pl.semaphore_wait(barrier, n_dev - 1)

    def send_kv(kind, s):
        src, dst = ((k_in, k_all), (v_in, v_all))[kind]
        return remote(kind, s, src.at[ahead(s)], dst.at[0, chip], ahead(s), core)

    def send_q(kind, s, t):
        src, dst = ((q_in, q_all), (do_in, do_all))[kind - Q]
        return remote(kind, 2 * s + t, src.at[ahead(s), t], dst.at[chip, t], ahead(s), lax.rem(core + t, 2))

    own_copies = (local(K, 0, k_in.at[chip], k_all.at[0, chip]), local(V, 0, v_in.at[chip], v_all.at[0, chip]),
                  local(Q, 0, q_in.at[chip, 0], q_all.at[chip, 0]), local(DO, 0, do_in.at[chip, 0], do_all.at[chip, 0]))
    sends = []
    for s in (1, 3, 2):
        sends += [send_kv(K, s), send_kv(V, s)]
    for pair in ((1, 3), (2,)):
        for kind in (Q, DO):
            sends += [send_q(kind, s, t) for s in pair for t in range(2)]
    sends += [send_q(Q, 0, 1), send_q(DO, 0, 1)]
    for copy in own_copies:
        copy.start()
    for copy in sends:
        copy.start()

    def zero_body(m, carry):
        for side in range(2):
            dk_all[side, m] = jnp.zeros((chunk, dim), jnp.float32)
            dv_all[side, m] = jnp.zeros((chunk, dim), jnp.float32)
        return carry
    lax.fori_loop(0, n_chip, zero_body, 0)

    def pass_on(kind, s):
        ref = (k_all, v_all)[kind - KX]
        return remote(kind, s, ref.at[0, behind(s)], ref.at[1, behind(s)], chip, 1 - core)

    def own_side(i, carry):
        s = order(i)
        m = behind(s)

        @pl.when(i == 0)
        def _():
            own_copies[0].wait()
            own_copies[1].wait()

        @pl.when(i > 0)
        def _():
            remote(K, s, k_in.at[0], k_all.at[0, m], chip, core).wait_recv()
            remote(V, s, v_in.at[0], v_all.at[0, m], chip, core).wait_recv()
        pass_on(KX, s).start()
        pass_on(VX, s).start()
        kt_all[0, m] = jnp.transpose(k_all[0, m])
        return carry
    lax.fori_loop(0, n_chip, own_side, 0)

    def other_side(i, carry):
        s = order(i)
        m = behind(s)
        pass_on(KX, s).wait_recv()
        pass_on(VX, s).wait_recv()
        kt_all[1, m] = jnp.transpose(k_all[1, m])
        return carry
    lax.fori_loop(0, n_chip, other_side, 0)

    def kv_slot(kb):
        chk = kb // n_half
        rows = pl.ds(pl.multiple_of(lax.rem(kb, n_half) * blk_len, blk_len), blk_len)
        return lax.rem(chk + core, 2), chk // 2, rows

    tok_q = lax.rem(lax.broadcasted_iota(jnp.int32, (rows2, blk_len), 0), blk_len)
    tok_k = lax.broadcasted_iota(jnp.int32, (rows2, blk_len), 1)
    tok_qt = lax.rem(lax.broadcasted_iota(jnp.int32, (blk_len, rows2), 1), blk_len)
    tok_kt = lax.broadcasted_iota(jnp.int32, (blk_len, rows2), 0)

    def block_of(s, u):
        return 2 * n_half * behind(s) + 2 * core + u * (3 - 4 * core)

    def fwd_task(s, u):
        m, idx = behind(s), 2 * s + u
        is_own = idx == 0

        @pl.when(is_own)
        def _():
            own_copies[2].wait()

        @pl.when(jnp.logical_not(is_own))
        def _():
            remote(Q, idx, q_in.at[0, 0], q_all.at[m, u], chip, core).wait_recv()

        blk = block_of(s, u)

        def fwd(kb, kind):
            side, mk, krows = kv_slot(kb)
            sc = dot_nt(q_all[m, u].reshape(rows2, dim), k_all[side, mk, krows, :])
            if kind == 'diag':
                sc = jnp.where(tok_k <= tok_q, sc, NEG_BIG)
            elif kind == 'far':
                sc = jnp.where(tok_k > tok_q, sc, NEG_BIG)
            s_max = jnp.max(sc, axis=1, keepdims=True)
            if kind == 'diag':
                m_new = jnp.broadcast_to(s_max, (rows2, 128))
            else:
                m_old = m_ref[...]
                m_new = jnp.maximum(m_old, s_max)
                alpha = jnp.exp2((m_old - m_new) * coef)
            p = jnp.exp2(sc * coef - (m_new * coef)[:, :1])
            p_sum = jnp.sum(p, axis=1, keepdims=True)
            pv = dot_nn(p.astype(jnp.bfloat16), v_all[side, mk, krows, :])
            m_ref[...] = m_new
            if kind == 'diag':
                l_ref[...] = jnp.broadcast_to(p_sum, (rows2, 128))
                acc_ref[...] = pv
            else:
                l_ref[...] = l_ref[...] * alpha + p_sum
                acc_ref[...] = acc_ref[...] * alpha[:, :1] + pv

        fwd(blk, 'diag')
        lax.fori_loop(jnp.maximum(blk - win + 1, 0), blk, lambda kb, c: (fwd(kb, 'full'), c)[1], 0)
        pl.when(blk >= win)(lambda: fwd(blk - win, 'far'))

        l_tot = l_ref[...]
        o_all[m, u] = (acc_ref[...] * (1.0 / l_tot)[:, :1]).astype(jnp.bfloat16).reshape(n_grp, blk_len, dim)
        stat_ref[idx, 0:1, :] = jnp.transpose(m_ref[...] * coef + jnp.log2(l_tot))[0:1, :]
        send_back(O, s, u)

    def send_back(kind, s, u):
        buf, out = ((o_all, o_out), (dq_all, dq_out))[kind - O]
        m, idx = behind(s), 2 * s + u

        @pl.when(idx == 0)
        def _():
            local(kind, 0, buf.at[chip, 0], out.at[chip, 0]).start()

        @pl.when(idx > 0)
        def _():
            remote(kind, idx, buf.at[m, u], out.at[chip, u], m, lax.rem(core + u, 2)).start()

    def bwd_unit(s, u, kv_chip, first, last):
        m, idx = behind(s), 2 * s + u
        blk = block_of(s, u)

        @pl.when(first)
        def _():
            @pl.when(idx == 0)
            def _():
                own_copies[3].wait()

            @pl.when(idx > 0)
            def _():
                remote(DO, idx, do_in.at[0, 0], do_all.at[m, u], chip, core).wait_recv()
            both = do_all[m, u].reshape(rows2, dim).astype(jnp.float32) * o_all[m, u].reshape(rows2, dim).astype(jnp.float32)
            drow = jnp.sum(both, axis=1, keepdims=True)
            stat_ref[idx, 1:2, :] = jnp.transpose(jnp.broadcast_to(drow, (rows2, 128)))[0:1, :]
            dqt_ref[u] = jnp.zeros((dim, rows2), jnp.float32)

        def bwd(kb, kind):
            side, mk, krows = kv_slot(kb)
            q2 = q_all[m, u].reshape(rows2, dim)
            do2 = do_all[m, u].reshape(rows2, dim)
            st = dot_nt(k_all[side, mk, krows, :], q2)
            if kind == 'diag':
                st = jnp.where(tok_kt <= tok_qt, st, NEG_BIG)
            elif kind == 'far':
                st = jnp.where(tok_kt > tok_qt, st, NEG_BIG)
            dpt = dot_nt(v_all[side, mk, krows, :], do2)
            p = jnp.exp2(st * coef - stat_ref[idx, 0:1, :])
            ds = (p * (dpt - stat_ref[idx, 1:2, :])).astype(jnp.bfloat16)
            dv_all[side, mk, krows, :] += dot_nn(p.astype(jnp.bfloat16), do2)
            dk_all[side, mk, krows, :] += dot_nn(ds, q2)
            dqt_ref[u] += dot_nn(kt_all[side, mk, :, krows], ds)

        per_chip = 2 * n_half
        pl.when(jnp.logical_and(blk >= win, (blk - win + per_chip) // per_chip == kv_chip + 1))(lambda: bwd(blk - win, 'far'))
        lo = jnp.maximum(jnp.maximum(blk - win + 1, 0), per_chip * kv_chip)
        hi = jnp.minimum(blk, per_chip * kv_chip + per_chip)
        lax.fori_loop(lo, hi, lambda kb, c: (bwd(kb, 'full'), c)[1], 0)
        pl.when(kv_chip == m)(lambda: bwd(blk, 'diag'))

        @pl.when(last)
        def _():
            dq_all[m, u] = jnp.transpose(dqt_ref[u] * scale).astype(jnp.bfloat16).reshape(n_grp, blk_len, dim)
            send_back(DQ, s, u)

    def swap(kind, s):
        src, dst = ((dk_all, dkx), (dv_all, dvx))[kind - DKX]
        return remote(kind, s, src.at[1, behind(s)], dst.at[behind(s)], chip, 1 - core)

    def swap_start(s):
        swap(DKX, s).start()
        swap(DVX, s).start()

    def settle(s):
        m = behind(s)
        for kind, part, other, buf, out, mul in ((DK, dk_all, dkx, k_all, dk_out, scale), (DV, dv_all, dvx, v_all, dv_out, 1.0)):
            swap(kind + 2, s).wait_recv()
            pass_on(kind - DK + KX, s).wait_send()

            def add_body(r, carry):
                rows = pl.ds(pl.multiple_of(r * 256, 256), 256)
                buf[0, m, rows, :] = ((part[0, m, rows, :] + other[m, rows, :]) * mul).astype(jnp.bfloat16)
                return carry
            lax.fori_loop(0, chunk // 256, add_body, 0)

            @pl.when(s == 0)
            def _():
                local(kind, 0, buf.at[0, chip], out.at[chip]).start()

            @pl.when(s > 0)
            def _():
                remote(kind, s, buf.at[0, m], out.at[chip], m, core).start()

    n_span = WINDOW // (2 * chunk) + 1
    n_task = 4 * n_chip

    def task_body(step, carry):
        task, half = step // 2, lax.rem(step, 2)
        is_fwd = jnp.logical_or(task < 3, task == 5)
        s = jnp.where(task < 3, order(task), jnp.where(task < 5, order(task - 2), jnp.where(task < 7, 2, 0)))
        pl.when(is_fwd)(lambda: fwd_task(s, half))

        @pl.when(jnp.logical_not(is_fwd))
        def _():
            own = s == 0

            def unit_body(j, carry):
                k = half * n_span + j
                u = jnp.where(own, lax.rem(k, 2), half)
                y = jnp.where(own, k // 2, j)

                @pl.when(jnp.logical_and(own, k == 0))
                def _():
                    swap_start(n_chip - 1)

                bwd_unit(s, u, behind(s) - n_span + 1 + y, y == 0, y == n_span - 1)

                @pl.when(own)
                def _():
                    @pl.when(lax.rem(k, 2) == 1)
                    def _():
                        swap_start(n_span - 1 - y)

                    @pl.when(lax.rem(k, 2) == 0)
                    def _():
                        settle(lax.rem(n_span - y, n_chip))
                return carry
            lax.fori_loop(0, n_span, unit_body, 0)
        return carry

    lax.fori_loop(0, n_task, task_body, 0)
    settle(0)

    for copy in sends:
        copy.wait_send()
    for s in range(n_chip):
        m = behind(s)
        h = ahead(s)
        swap(DKX, s).wait_send()
        swap(DVX, s).wait_send()
        for kind, buf, out in ((O, o_all, o_out), (DQ, dq_all, dq_out)):
            for t in range(2):
                if s == 0 and t == 0:
                    local(kind, 0, buf.at[chip, 0], out.at[chip, 0]).wait()
                else:
                    remote(kind, 2 * s + t, buf.at[m, t], out.at[chip, t], m, lax.rem(core + t, 2)).wait_send()
                    remote(kind, 2 * s + t, buf.at[m, t], out.at[h, t], m, core).wait_recv()
        for kind, buf, out in ((DK, k_all, dk_out), (DV, v_all, dv_out)):
            if s == 0:
                local(kind, 0, buf.at[0, chip], out.at[chip]).wait()
            else:
                remote(kind, s, buf.at[0, m], out.at[chip], m, core).wait_send()
                remote(kind, s, buf.at[0, m], out.at[h], m, core).wait_recv()


def solution(mesh):
    n_chip = mesh.shape['ctx'] // 2
    seq_spec = P('dp', 'ctx', None, None)

    def local_attn(q_loc, k_loc, v_loc, do_loc):
        _, chunk, q_heads, dim = q_loc.shape
        kv_heads = k_loc.shape[2]
        n_grp = q_heads // kv_heads
        blk_len = chunk // 2
        rows = n_grp * blk_len
        bf16, f32 = jnp.bfloat16, jnp.float32

        def split_q(x):
            return jnp.transpose(x.reshape(2, blk_len, kv_heads, n_grp, dim), (2, 0, 3, 1, 4))

        def split_kv(x):
            return jnp.transpose(x.reshape(chunk, kv_heads, dim), (1, 0, 2))

        q_shape, kv_shape = (n_chip, 2, n_grp, blk_len, dim), (n_chip, chunk, dim)
        q_type, kv_type = jax.ShapeDtypeStruct(q_shape, bf16), jax.ShapeDtypeStruct(kv_shape, bf16)
        o_all, dq_all, dk_all, dv_all = pl.pallas_call(
            attn_kernel,
            out_shape=(q_type, q_type, kv_type, kv_type),
            in_specs=[pl.BlockSpec(memory_space=pl.ANY)] * 4,
            out_specs=[pl.BlockSpec(memory_space=pl.ANY)] * 4,
            scratch_shapes=[
                pltpu.VMEM(q_shape, bf16),
                pltpu.VMEM(q_shape, bf16),
                pltpu.VMEM((2,) + kv_shape, bf16),
                pltpu.VMEM((2,) + kv_shape, bf16),
                pltpu.VMEM((2, n_chip, dim, chunk), bf16),
                pltpu.VMEM((2,) + kv_shape, f32),
                pltpu.VMEM((2,) + kv_shape, f32),
                pltpu.VMEM(q_shape, bf16),
                pltpu.VMEM(q_shape, bf16),
                pltpu.VMEM(kv_shape, f32),
                pltpu.VMEM(kv_shape, f32),
                pltpu.VMEM((rows, dim), f32),
                pltpu.VMEM((rows, 128), f32),
                pltpu.VMEM((rows, 128), f32),
                pltpu.VMEM((2 * n_chip, 8, rows), f32),
                pltpu.VMEM((2, dim, rows), f32),
                pltpu.SemaphoreType.DMA((12, 8)),
                pltpu.SemaphoreType.DMA((12, 8)),
            ],
            compiler_params=pltpu.CompilerParams(vmem_limit_bytes=67043328, collective_id=0, has_side_effects=True),
        )(split_q(q_loc), split_q(do_loc), split_kv(k_loc), split_kv(v_loc))

        def join_q(x):
            return jnp.transpose(x, (1, 3, 0, 2, 4)).reshape(q_loc.shape)

        def join_kv(x):
            return jnp.transpose(x, (1, 0, 2)).reshape(k_loc.shape)

        return join_q(o_all), join_q(dq_all), join_kv(dk_all), join_kv(dv_all)

    return jax.shard_map(local_attn, mesh=mesh, in_specs=(seq_spec,) * 4, out_specs=(seq_spec,) * 4, check_vma=False)
```

```python
import math

import jax
import jax.numpy as jnp
from jax import lax
from jax.experimental import pallas as pl
from jax.experimental.pallas import tpu as pltpu
from jax.sharding import PartitionSpec as P

WINDOW = 4096
NEG_BIG = -1e30
COLS = 256
MESH = pl.DeviceIdType.MESH
K, V, KX, VX, Q, DO, O, DQ, DK, DV, DKX, DVX = range(12)


def dot_nn(a, b):
    return lax.dot_general(a, b, (((1,), (0,)), ((), ())), preferred_element_type=jnp.float32)


def dot_nt(a, b):
    return lax.dot_general(a, b, (((1,), (1,)), ((), ())), preferred_element_type=jnp.float32)


def dot_tn(a, b):
    return lax.dot_general(a, b, (((0,), (0,)), ((), ())), preferred_element_type=jnp.float32)


def attn_kernel(q_in, do_in, k_in, v_in, o_out, dq_out, dk_out, dv_out,
                q_all, do_all, k_all, v_all, kt_all, dk_all, dv_all, o_all, dq_all, dkx, dvx,
                acc_ref, max_ref, sum_ref, stat_ref, dqt_ref, send_sem, recv_sem):
    n_chip, n_half, n_grp, blk_len, dim = q_all.shape
    chunk = n_half * blk_len
    n_dev = 2 * n_chip
    rows2 = n_grp * blk_len
    me = lax.axis_index('ctx')
    chip, core = me // 2, lax.rem(me, 2)
    win = WINDOW // blk_len
    scale = dim ** -0.5
    coef = scale * math.log2(math.e)

    def order(i):
        return i + i // 2 - 2 * (i // 3)

    def ahead(s):
        return lax.rem(chip + s, n_chip)

    def behind(s):
        return lax.rem(chip + n_chip - s, n_chip)

    def remote(kind, idx, src, dst, to_chip, to_core):
        return pltpu.make_async_remote_copy(
            src_ref=src, dst_ref=dst, send_sem=send_sem.at[kind, idx], recv_sem=recv_sem.at[kind, idx],
            device_id={'ctx': 2 * to_chip + to_core}, device_id_type=MESH)

    def local(kind, idx, src, dst):
        return pltpu.make_async_copy(src, dst, recv_sem.at[kind, idx])

    barrier = pltpu.get_barrier_semaphore()
    for step in range(1, n_dev):
        pl.semaphore_signal(barrier, inc=1, device_id={'ctx': lax.rem(me + step, n_dev)}, device_id_type=MESH)
    pl.semaphore_wait(barrier, n_dev - 1)

    def part(ref, g, t):
        return ref.at[g, :, pl.ds(pl.multiple_of(t * blk_len, blk_len), blk_len), :]

    def send_kv(kind, s):
        src, dst = ((k_in, k_all), (v_in, v_all))[kind]
        return remote(kind, s, src.at[ahead(s)], dst.at[0, chip], ahead(s), core)

    def send_q(kind, s, t):
        src, dst = ((q_in, q_all), (do_in, do_all))[kind - Q]
        return remote(kind, 2 * s + t, part(src, ahead(s), t), dst.at[chip, t], ahead(s), lax.rem(core + t, 2))

    own_copies = (local(K, 0, k_in.at[chip], k_all.at[0, chip]), local(V, 0, v_in.at[chip], v_all.at[0, chip]),
                  local(Q, 0, part(q_in, chip, 0), q_all.at[chip, 0]), local(DO, 0, part(do_in, chip, 0), do_all.at[chip, 0]))
    sends = []
    for s in (1, 3, 2):
        sends += [send_kv(K, s), send_kv(V, s)]
    for pair in ((1, 3), (2,)):
        for kind in (Q, DO):
            sends += [send_q(kind, s, t) for s in pair for t in range(2)]
    sends += [send_q(Q, 0, 1), send_q(DO, 0, 1)]
    for copy in own_copies:
        copy.start()
    for copy in sends:
        copy.start()

    def zero_body(m, carry):
        for side in range(2):
            dk_all[side, m] = jnp.zeros((chunk, dim), jnp.float32)
            dv_all[side, m] = jnp.zeros((chunk, dim), jnp.float32)
        return carry
    lax.fori_loop(0, n_chip, zero_body, 0)

    def pass_on(kind, s):
        ref = (k_all, v_all)[kind - KX]
        return remote(kind, s, ref.at[0, behind(s)], ref.at[1, behind(s)], chip, 1 - core)

    def own_side(i, carry):
        s = order(i)
        m = behind(s)

        @pl.when(i == 0)
        def _():
            own_copies[0].wait()
            own_copies[1].wait()

        @pl.when(i > 0)
        def _():
            remote(K, s, k_in.at[0], k_all.at[0, m], chip, core).wait_recv()
            remote(V, s, v_in.at[0], v_all.at[0, m], chip, core).wait_recv()
        pass_on(KX, s).start()
        pass_on(VX, s).start()
        kt_all[0, m] = jnp.transpose(k_all[0, m])
        return carry
    lax.fori_loop(0, n_chip, own_side, 0)

    def other_side(i, carry):
        s = order(i)
        m = behind(s)
        pass_on(KX, s).wait_recv()
        pass_on(VX, s).wait_recv()
        kt_all[1, m] = jnp.transpose(k_all[1, m])
        return carry
    lax.fori_loop(0, n_chip, other_side, 0)

    def kv_slot(kb):
        chk = kb // n_half
        rows = pl.ds(pl.multiple_of(lax.rem(kb, n_half) * blk_len, blk_len), blk_len)
        return lax.rem(chk + core, 2), chk // 2, rows

    tok_qt = lax.rem(lax.broadcasted_iota(jnp.int32, (blk_len, rows2), 1), blk_len)
    tok_kt = lax.broadcasted_iota(jnp.int32, (blk_len, rows2), 0)

    def block_of(s, u):
        return 2 * n_half * behind(s) + 2 * core + u * (3 - 4 * core)

    def fwd_task(s, u):
        m, idx = behind(s), 2 * s + u
        is_own = idx == 0

        @pl.when(is_own)
        def _():
            own_copies[2].wait()

        @pl.when(jnp.logical_not(is_own))
        def _():
            remote(Q, idx, part(q_in, 0, 0), q_all.at[m, u], chip, core).wait_recv()

        blk = block_of(s, u)

        def fwd(kb, kind):
            side, mk, krows = kv_slot(kb)
            q2 = q_all[m, u].reshape(rows2, dim)
            k_blk, v_blk = k_all[side, mk, krows, :], v_all[side, mk, krows, :]
            cols = [slice(c * COLS, (c + 1) * COLS) for c in range(rows2 // COLS)]

            def scores(c):
                st = dot_nt(k_blk, q2[c])
                if kind == 'diag':
                    st = jnp.where(tok_kt[:, c] <= tok_qt[:, c], st, NEG_BIG)
                elif kind == 'far':
                    st = jnp.where(tok_kt[:, c] > tok_qt[:, c], st, NEG_BIG)
                return st

            def weigh(c, st):
                m_new = jnp.max(st, axis=0, keepdims=True)
                if kind != 'diag':
                    m_old = max_ref[:, c]
                    m_new = jnp.maximum(m_old, m_new)
                    alpha = jnp.exp2((m_old - m_new) * coef)
                p = jnp.exp2(st * coef - m_new * coef)
                p_sum = jnp.sum(p, axis=0, keepdims=True)
                pv = dot_tn(v_blk, p.astype(jnp.bfloat16))
                max_ref[:, c] = m_new
                if kind == 'diag':
                    sum_ref[:, c] = p_sum
                    acc_ref[:, c] = pv
                else:
                    sum_ref[:, c] = sum_ref[:, c] * alpha + p_sum
                    acc_ref[:, c] = acc_ref[:, c] * alpha + pv

            ready = scores(cols[0])
            for here, after in zip(cols, cols[1:] + [None]):
                then = scores(after) if after is not None else None
                weigh(here, ready)
                ready = then

        fwd(blk, 'diag')
        lax.fori_loop(jnp.maximum(blk - win + 1, 0), blk, lambda kb, c: (fwd(kb, 'full'), c)[1], 0)
        pl.when(blk >= win)(lambda: fwd(blk - win, 'far'))

        total = sum_ref[...]
        o_all[m, u] = jnp.transpose(acc_ref[...] * (1.0 / total)).astype(jnp.bfloat16).reshape(n_grp, blk_len, dim)
        stat_ref[idx, 0:1, :] = max_ref[...] * coef + jnp.log2(total)
        send_back(O, s, u)

    def send_back(kind, s, u):
        buf, out = ((o_all, o_out), (dq_all, dq_out))[kind - O]
        m, idx = behind(s), 2 * s + u

        @pl.when(idx == 0)
        def _():
            local(kind, 0, buf.at[chip, 0], part(out, chip, 0)).start()

        @pl.when(idx > 0)
        def _():
            remote(kind, idx, buf.at[m, u], part(out, chip, u), m, lax.rem(core + u, 2)).start()

    def bwd_unit(s, u, kv_chip, first, last):
        m, idx = behind(s), 2 * s + u
        blk = block_of(s, u)

        @pl.when(first)
        def _():
            @pl.when(idx == 0)
            def _():
                own_copies[3].wait()

            @pl.when(idx > 0)
            def _():
                remote(DO, idx, part(do_in, 0, 0), do_all.at[m, u], chip, core).wait_recv()
            both = do_all[m, u].reshape(rows2, dim).astype(jnp.float32) * o_all[m, u].reshape(rows2, dim).astype(jnp.float32)
            drow = jnp.sum(both, axis=1, keepdims=True)
            stat_ref[idx, 1:2, :] = jnp.transpose(jnp.broadcast_to(drow, (rows2, 128)))[0:1, :]
            dqt_ref[u] = jnp.zeros((dim, rows2), jnp.float32)

        def bwd(kb, kind):
            side, mk, krows = kv_slot(kb)
            q2 = q_all[m, u].reshape(rows2, dim)
            do2 = do_all[m, u].reshape(rows2, dim)
            st = dot_nt(k_all[side, mk, krows, :], q2)
            if kind == 'diag':
                st = jnp.where(tok_kt <= tok_qt, st, NEG_BIG)
            elif kind == 'far':
                st = jnp.where(tok_kt > tok_qt, st, NEG_BIG)
            dpt = dot_nt(v_all[side, mk, krows, :], do2)
            p = jnp.exp2(st * coef - stat_ref[idx, 0:1, :])
            ds = (p * (dpt - stat_ref[idx, 1:2, :])).astype(jnp.bfloat16)
            dv_all[side, mk, krows, :] += dot_nn(p.astype(jnp.bfloat16), do2)
            dk_all[side, mk, krows, :] += dot_nn(ds, q2)
            dqt_ref[u] += dot_nn(kt_all[side, mk, :, krows], ds)

        per_chip = 2 * n_half
        pl.when(jnp.logical_and(blk >= win, (blk - win + per_chip) // per_chip == kv_chip + 1))(lambda: bwd(blk - win, 'far'))
        lo = jnp.maximum(jnp.maximum(blk - win + 1, 0), per_chip * kv_chip)
        hi = jnp.minimum(blk, per_chip * kv_chip + per_chip)
        lax.fori_loop(lo, hi, lambda kb, c: (bwd(kb, 'full'), c)[1], 0)
        pl.when(kv_chip == m)(lambda: bwd(blk, 'diag'))

        @pl.when(last)
        def _():
            dq_all[m, u] = jnp.transpose(dqt_ref[u] * scale).astype(jnp.bfloat16).reshape(n_grp, blk_len, dim)
            send_back(DQ, s, u)

    def swap(kind, s):
        src, dst = ((dk_all, dkx), (dv_all, dvx))[kind - DKX]
        return remote(kind, s, src.at[1, behind(s)], dst.at[behind(s)], chip, 1 - core)

    def swap_start(s):
        swap(DKX, s).start()
        swap(DVX, s).start()

    def settle(s):
        m = behind(s)
        for kind, mine, other, buf, out, mul in ((DK, dk_all, dkx, k_all, dk_out, scale), (DV, dv_all, dvx, v_all, dv_out, 1.0)):
            swap(kind + 2, s).wait_recv()
            pass_on(kind - DK + KX, s).wait_send()

            def add_body(r, carry):
                rows = pl.ds(pl.multiple_of(r * 256, 256), 256)
                buf[0, m, rows, :] = ((mine[0, m, rows, :] + other[m, rows, :]) * mul).astype(jnp.bfloat16)
                return carry
            lax.fori_loop(0, chunk // 256, add_body, 0)

            @pl.when(s == 0)
            def _():
                local(kind, 0, buf.at[0, chip], out.at[chip]).start()

            @pl.when(s > 0)
            def _():
                remote(kind, s, buf.at[0, m], out.at[chip], m, core).start()

    n_span = WINDOW // (2 * chunk) + 1
    n_task = 4 * n_chip

    def task_body(step, carry):
        task, half = step // 2, lax.rem(step, 2)
        is_fwd = jnp.logical_or(task < 3, task == 5)
        s = jnp.where(task < 3, order(task), jnp.where(task < 5, order(task - 2), jnp.where(task < 7, 2, 0)))
        pl.when(is_fwd)(lambda: fwd_task(s, half))

        @pl.when(jnp.logical_not(is_fwd))
        def _():
            own = s == 0

            def unit_body(j, carry):
                k = half * n_span + j
                u = jnp.where(own, lax.rem(k, 2), half)
                y = jnp.where(own, k // 2, j)

                @pl.when(jnp.logical_and(own, k == 0))
                def _():
                    swap_start(n_chip - 1)

                bwd_unit(s, u, behind(s) - n_span + 1 + y, y == 0, y == n_span - 1)

                @pl.when(own)
                def _():
                    @pl.when(lax.rem(k, 2) == 1)
                    def _():
                        swap_start(n_span - 1 - y)

                    @pl.when(lax.rem(k, 2) == 0)
                    def _():
                        settle(lax.rem(n_span - y, n_chip))
                return carry
            lax.fori_loop(0, n_span, unit_body, 0)
        return carry

    lax.fori_loop(0, n_task, task_body, 0)
    settle(0)

    for copy in sends:
        copy.wait_send()
    for s in range(n_chip):
        m = behind(s)
        h = ahead(s)
        swap(DKX, s).wait_send()
        swap(DVX, s).wait_send()
        for kind, buf, out in ((O, o_all, o_out), (DQ, dq_all, dq_out)):
            for t in range(2):
                if s == 0 and t == 0:
                    local(kind, 0, buf.at[chip, 0], part(out, chip, 0)).wait()
                else:
                    remote(kind, 2 * s + t, buf.at[m, t], part(out, chip, t), m, lax.rem(core + t, 2)).wait_send()
                    remote(kind, 2 * s + t, buf.at[m, t], part(out, h, t), m, core).wait_recv()
        for kind, buf, out in ((DK, k_all, dk_out), (DV, v_all, dv_out)):
            if s == 0:
                local(kind, 0, buf.at[0, chip], out.at[chip]).wait()
            else:
                remote(kind, s, buf.at[0, m], out.at[chip], m, core).wait_send()
                remote(kind, s, buf.at[0, m], out.at[h], m, core).wait_recv()


def solution(mesh):
    n_chip = mesh.shape['ctx'] // 2
    seq_spec = P('dp', 'ctx', None, None)

    def local_attn(q_loc, k_loc, v_loc, do_loc):
        _, chunk, q_heads, dim = q_loc.shape
        kv_heads = k_loc.shape[2]
        n_grp = q_heads // kv_heads
        blk_len = chunk // 2
        rows = n_grp * blk_len
        bf16, f32 = jnp.bfloat16, jnp.float32

        def split_q(x):
            return jnp.transpose(x.reshape(chunk, kv_heads, n_grp, dim), (1, 2, 0, 3))

        def split_kv(x):
            return jnp.transpose(x.reshape(chunk, kv_heads, dim), (1, 0, 2))

        q_shape, kv_shape = (n_chip, 2, n_grp, blk_len, dim), (n_chip, chunk, dim)
        q_type, kv_type = jax.ShapeDtypeStruct((n_chip, n_grp, chunk, dim), bf16), jax.ShapeDtypeStruct(kv_shape, bf16)
        o_all, dq_all, dk_all, dv_all = pl.pallas_call(
            attn_kernel,
            out_shape=(q_type, q_type, kv_type, kv_type),
            in_specs=[pl.BlockSpec(memory_space=pl.ANY)] * 4,
            out_specs=[pl.BlockSpec(memory_space=pl.ANY)] * 4,
            scratch_shapes=[
                pltpu.VMEM(q_shape, bf16),
                pltpu.VMEM(q_shape, bf16),
                pltpu.VMEM((2,) + kv_shape, bf16),
                pltpu.VMEM((2,) + kv_shape, bf16),
                pltpu.VMEM((2, n_chip, dim, chunk), bf16),
                pltpu.VMEM((2,) + kv_shape, f32),
                pltpu.VMEM((2,) + kv_shape, f32),
                pltpu.VMEM(q_shape, bf16),
                pltpu.VMEM(q_shape, bf16),
                pltpu.VMEM(kv_shape, f32),
                pltpu.VMEM(kv_shape, f32),
                pltpu.VMEM((dim, rows), f32),
                pltpu.VMEM((1, rows), f32),
                pltpu.VMEM((1, rows), f32),
                pltpu.VMEM((2 * n_chip, 8, rows), f32),
                pltpu.VMEM((2, dim, rows), f32),
                pltpu.SemaphoreType.DMA((12, 8)),
                pltpu.SemaphoreType.DMA((12, 8)),
            ],
            compiler_params=pltpu.CompilerParams(vmem_limit_bytes=67043328, collective_id=0, has_side_effects=True),
        )(split_q(q_loc), split_q(do_loc), split_kv(k_loc), split_kv(v_loc))

        def join_q(x):
            return jnp.transpose(x, (2, 0, 1, 3)).reshape(q_loc.shape)

        def join_kv(x):
            return jnp.transpose(x, (1, 0, 2)).reshape(k_loc.shape)

        return join_q(o_all), join_q(dq_all), join_kv(dk_all), join_kv(dv_all)

    return jax.shard_map(local_attn, mesh=mesh, in_specs=(seq_spec,) * 4, out_specs=(seq_spec,) * 4, check_vma=False)
```

```python
import math

import jax
import jax.numpy as jnp
from jax import lax
from jax.experimental import pallas as pl
from jax.experimental.pallas import tpu as pltpu
from jax.sharding import PartitionSpec as P

WINDOW = 4096
NEG_BIG = -1e30
COLS = 512
MESH = pl.DeviceIdType.MESH
K, V, KX, VX, Q, DO, O, DQ, DK, DV, DKX, DVX = range(12)


def dot_nn(a, b):
    return lax.dot_general(a, b, (((1,), (0,)), ((), ())), preferred_element_type=jnp.float32)


def dot_nt(a, b):
    return lax.dot_general(a, b, (((1,), (1,)), ((), ())), preferred_element_type=jnp.float32)


def dot_tn(a, b):
    return lax.dot_general(a, b, (((0,), (0,)), ((), ())), preferred_element_type=jnp.float32)


def attn_kernel(q_in, do_in, k_in, v_in, o_out, dq_out, dk_out, dv_out,
                q_all, do_all, k_all, v_all, kt_all, dk_all, dv_all, o_all, dq_all, dkx, dvx,
                acc_ref, s_ref, max_ref, sum_ref, stat_ref, dqt_ref, send_sem, recv_sem):
    n_chip, n_half, n_grp, blk_len, dim = q_all.shape
    chunk = n_half * blk_len
    n_dev = 2 * n_chip
    rows2 = n_grp * blk_len
    me = lax.axis_index('ctx')
    chip, core = me // 2, lax.rem(me, 2)
    win = WINDOW // blk_len
    scale = dim ** -0.5
    coef = scale * math.log2(math.e)

    def order(i):
        return i + i // 2 - 2 * (i // 3)

    def ahead(s):
        return lax.rem(chip + s, n_chip)

    def behind(s):
        return lax.rem(chip + n_chip - s, n_chip)

    def remote(kind, idx, src, dst, to_chip, to_core):
        return pltpu.make_async_remote_copy(
            src_ref=src, dst_ref=dst, send_sem=send_sem.at[kind, idx], recv_sem=recv_sem.at[kind, idx],
            device_id={'ctx': 2 * to_chip + to_core}, device_id_type=MESH)

    def local(kind, idx, src, dst):
        return pltpu.make_async_copy(src, dst, recv_sem.at[kind, idx])

    barrier = pltpu.get_barrier_semaphore()
    for step in range(1, n_dev):
        pl.semaphore_signal(barrier, inc=1, device_id={'ctx': lax.rem(me + step, n_dev)}, device_id_type=MESH)
    pl.semaphore_wait(barrier, n_dev - 1)

    def part(ref, g, t):
        return ref.at[g, :, pl.ds(pl.multiple_of(t * blk_len, blk_len), blk_len), :]

    def send_kv(kind, s):
        src, dst = ((k_in, k_all), (v_in, v_all))[kind]
        return remote(kind, s, src.at[ahead(s)], dst.at[0, chip], ahead(s), core)

    def send_q(kind, s, t):
        src, dst = ((q_in, q_all), (do_in, do_all))[kind - Q]
        return remote(kind, 2 * s + t, part(src, ahead(s), t), dst.at[chip, t], ahead(s), lax.rem(core + t, 2))

    own_copies = (local(K, 0, k_in.at[chip], k_all.at[0, chip]), local(V, 0, v_in.at[chip], v_all.at[0, chip]),
                  local(Q, 0, part(q_in, chip, 0), q_all.at[chip, 0]), local(DO, 0, part(do_in, chip, 0), do_all.at[chip, 0]))
    sends = []
    for s in (1, 3, 2):
        sends += [send_kv(K, s), send_kv(V, s)]
    for pair in ((1, 3), (2,)):
        for kind in (Q, DO):
            sends += [send_q(kind, s, t) for s in pair for t in range(2)]
    sends += [send_q(Q, 0, 1), send_q(DO, 0, 1)]
    for copy in own_copies:
        copy.start()
    for copy in sends:
        copy.start()

    def zero_body(m, carry):
        for side in range(2):
            dk_all[side, m] = jnp.zeros((chunk, dim), jnp.float32)
            dv_all[side, m] = jnp.zeros((chunk, dim), jnp.float32)
        return carry
    lax.fori_loop(0, n_chip, zero_body, 0)

    def pass_on(kind, s):
        ref = (k_all, v_all)[kind - KX]
        return remote(kind, s, ref.at[0, behind(s)], ref.at[1, behind(s)], chip, 1 - core)

    def own_side(i, carry):
        s = order(i)
        m = behind(s)

        @pl.when(i == 0)
        def _():
            own_copies[0].wait()
            own_copies[1].wait()

        @pl.when(i > 0)
        def _():
            remote(K, s, k_in.at[0], k_all.at[0, m], chip, core).wait_recv()
            remote(V, s, v_in.at[0], v_all.at[0, m], chip, core).wait_recv()
        pass_on(KX, s).start()
        pass_on(VX, s).start()
        kt_all[0, m] = jnp.transpose(k_all[0, m])
        return carry
    lax.fori_loop(0, n_chip, own_side, 0)

    def other_side(i, carry):
        s = order(i)
        m = behind(s)
        pass_on(KX, s).wait_recv()
        pass_on(VX, s).wait_recv()
        kt_all[1, m] = jnp.transpose(k_all[1, m])
        return carry
    lax.fori_loop(0, n_chip, other_side, 0)

    def kv_slot(kb):
        chk = kb // n_half
        rows = pl.ds(pl.multiple_of(lax.rem(kb, n_half) * blk_len, blk_len), blk_len)
        return lax.rem(chk + core, 2), chk // 2, rows

    tok_qt = lax.rem(lax.broadcasted_iota(jnp.int32, (blk_len, rows2), 1), blk_len)
    tok_kt = lax.broadcasted_iota(jnp.int32, (blk_len, rows2), 0)

    def block_of(s, u):
        return 2 * n_half * behind(s) + 2 * core + u * (3 - 4 * core)

    def fwd_task(s, u):
        m, idx = behind(s), 2 * s + u
        is_own = idx == 0

        @pl.when(is_own)
        def _():
            own_copies[2].wait()

        @pl.when(jnp.logical_not(is_own))
        def _():
            remote(Q, idx, part(q_in, 0, 0), q_all.at[m, u], chip, core).wait_recv()

        blk = block_of(s, u)

        def fwd(kb, kind, kb_next):
            side, mk, krows = kv_slot(kb)
            q2 = q_all[m, u].reshape(rows2, dim)
            v_blk = v_all[side, mk, krows, :]
            cols = [slice(c * COLS, (c + 1) * COLS) for c in range(rows2 // COLS)]

            def scores(kb_s, c):
                side_s, mk_s, krows_s = kv_slot(kb_s)
                return dot_nt(k_all[side_s, mk_s, krows_s, :], q2[c])

            for c in cols:
                st = scores(kb, c) if kind == 'diag' else s_ref[:, c]
                if kind == 'diag':
                    st = jnp.where(tok_kt[:, c] <= tok_qt[:, c], st, NEG_BIG)
                elif kind == 'far':
                    st = jnp.where(tok_kt[:, c] > tok_qt[:, c], st, NEG_BIG)
                if kb_next is not None:
                    s_ref[:, c] = scores(kb_next, c)
                m_new = jnp.max(st, axis=0, keepdims=True)
                if kind != 'diag':
                    m_old = max_ref[:, c]
                    m_new = jnp.maximum(m_old, m_new)
                    alpha = jnp.exp2((m_old - m_new) * coef)
                p = jnp.exp2(st * coef - m_new * coef)
                p_sum = jnp.sum(p, axis=0, keepdims=True)
                pv = dot_tn(v_blk, p.astype(jnp.bfloat16))
                max_ref[:, c] = m_new
                if kind == 'diag':
                    sum_ref[:, c] = p_sum
                    acc_ref[:, c] = pv
                else:
                    sum_ref[:, c] = sum_ref[:, c] * alpha + p_sum
                    acc_ref[:, c] = acc_ref[:, c] * alpha + pv

        lo = jnp.maximum(blk - win + 1, 0)
        far = jnp.maximum(blk - win, 0)
        fwd(blk, 'diag', jnp.where(lo < blk, lo, far))
        lax.fori_loop(lo, blk, lambda kb, c: (fwd(kb, 'full', jnp.where(kb + 1 < blk, kb + 1, far)), c)[1], 0)
        pl.when(blk >= win)(lambda: fwd(blk - win, 'far', None))

        total = sum_ref[...]
        o_all[m, u] = jnp.transpose(acc_ref[...] * (1.0 / total)).astype(jnp.bfloat16).reshape(n_grp, blk_len, dim)
        stat_ref[idx, 0:1, :] = max_ref[...] * coef + jnp.log2(total)
        send_back(O, s, u)

    def send_back(kind, s, u):
        buf, out = ((o_all, o_out), (dq_all, dq_out))[kind - O]
        m, idx = behind(s), 2 * s + u

        @pl.when(idx == 0)
        def _():
            local(kind, 0, buf.at[chip, 0], part(out, chip, 0)).start()

        @pl.when(idx > 0)
        def _():
            remote(kind, idx, buf.at[m, u], part(out, chip, u), m, lax.rem(core + u, 2)).start()

    def bwd_unit(s, u, kv_chip, first, last):
        m, idx = behind(s), 2 * s + u
        blk = block_of(s, u)

        @pl.when(first)
        def _():
            @pl.when(idx == 0)
            def _():
                own_copies[3].wait()

            @pl.when(idx > 0)
            def _():
                remote(DO, idx, part(do_in, 0, 0), do_all.at[m, u], chip, core).wait_recv()
            both = do_all[m, u].reshape(rows2, dim).astype(jnp.float32) * o_all[m, u].reshape(rows2, dim).astype(jnp.float32)
            drow = jnp.sum(both, axis=1, keepdims=True)
            stat_ref[idx, 1:2, :] = jnp.transpose(jnp.broadcast_to(drow, (rows2, 128)))[0:1, :]
            dqt_ref[u] = jnp.zeros((dim, rows2), jnp.float32)

        def bwd(kb, kind):
            side, mk, krows = kv_slot(kb)
            q2 = q_all[m, u].reshape(rows2, dim)
            do2 = do_all[m, u].reshape(rows2, dim)
            st = dot_nt(k_all[side, mk, krows, :], q2)
            if kind == 'diag':
                st = jnp.where(tok_kt <= tok_qt, st, NEG_BIG)
            elif kind == 'far':
                st = jnp.where(tok_kt > tok_qt, st, NEG_BIG)
            dpt = dot_nt(v_all[side, mk, krows, :], do2)
            p = jnp.exp2(st * coef - stat_ref[idx, 0:1, :])
            ds = (p * (dpt - stat_ref[idx, 1:2, :])).astype(jnp.bfloat16)
            dv_all[side, mk, krows, :] += dot_nn(p.astype(jnp.bfloat16), do2)
            dk_all[side, mk, krows, :] += dot_nn(ds, q2)
            dqt_ref[u] += dot_nn(kt_all[side, mk, :, krows], ds)

        per_chip = 2 * n_half
        pl.when(jnp.logical_and(blk >= win, (blk - win + per_chip) // per_chip == kv_chip + 1))(lambda: bwd(blk - win, 'far'))
        lo = jnp.maximum(jnp.maximum(blk - win + 1, 0), per_chip * kv_chip)
        hi = jnp.minimum(blk, per_chip * kv_chip + per_chip)
        lax.fori_loop(lo, hi, lambda kb, c: (bwd(kb, 'full'), c)[1], 0)
        pl.when(kv_chip == m)(lambda: bwd(blk, 'diag'))

        @pl.when(last)
        def _():
            dq_all[m, u] = jnp.transpose(dqt_ref[u] * scale).astype(jnp.bfloat16).reshape(n_grp, blk_len, dim)
            send_back(DQ, s, u)

    def swap(kind, s):
        src, dst = ((dk_all, dkx), (dv_all, dvx))[kind - DKX]
        return remote(kind, s, src.at[1, behind(s)], dst.at[behind(s)], chip, 1 - core)

    def swap_start(s):
        swap(DKX, s).start()
        swap(DVX, s).start()

    def settle(s):
        m = behind(s)
        for kind, mine, other, buf, out, mul in ((DK, dk_all, dkx, k_all, dk_out, scale), (DV, dv_all, dvx, v_all, dv_out, 1.0)):
            swap(kind + 2, s).wait_recv()
            pass_on(kind - DK + KX, s).wait_send()

            def add_body(r, carry):
                rows = pl.ds(pl.multiple_of(r * 256, 256), 256)
                buf[0, m, rows, :] = ((mine[0, m, rows, :] + other[m, rows, :]) * mul).astype(jnp.bfloat16)
                return carry
            lax.fori_loop(0, chunk // 256, add_body, 0)

            @pl.when(s == 0)
            def _():
                local(kind, 0, buf.at[0, chip], out.at[chip]).start()

            @pl.when(s > 0)
            def _():
                remote(kind, s, buf.at[0, m], out.at[chip], m, core).start()

    n_span = WINDOW // (2 * chunk) + 1
    n_task = 4 * n_chip

    def task_body(step, carry):
        task, half = step // 2, lax.rem(step, 2)
        is_fwd = jnp.logical_or(task < 3, task == 5)
        s = jnp.where(task < 3, order(task), jnp.where(task < 5, order(task - 2), jnp.where(task < 7, 2, 0)))
        pl.when(is_fwd)(lambda: fwd_task(s, half))

        @pl.when(jnp.logical_not(is_fwd))
        def _():
            own = s == 0

            def unit_body(j, carry):
                k = half * n_span + j
                u = jnp.where(own, lax.rem(k, 2), half)
                y = jnp.where(own, k // 2, j)

                @pl.when(jnp.logical_and(own, k == 0))
                def _():
                    swap_start(n_chip - 1)

                bwd_unit(s, u, behind(s) - n_span + 1 + y, y == 0, y == n_span - 1)

                @pl.when(own)
                def _():
                    @pl.when(lax.rem(k, 2) == 1)
                    def _():
                        swap_start(n_span - 1 - y)

                    @pl.when(lax.rem(k, 2) == 0)
                    def _():
                        settle(lax.rem(n_span - y, n_chip))
                return carry
            lax.fori_loop(0, n_span, unit_body, 0)
        return carry

    lax.fori_loop(0, n_task, task_body, 0)
    settle(0)

    for copy in sends:
        copy.wait_send()
    for s in range(n_chip):
        m = behind(s)
        h = ahead(s)
        swap(DKX, s).wait_send()
        swap(DVX, s).wait_send()
        for kind, buf, out in ((O, o_all, o_out), (DQ, dq_all, dq_out)):
            for t in range(2):
                if s == 0 and t == 0:
                    local(kind, 0, buf.at[chip, 0], part(out, chip, 0)).wait()
                else:
                    remote(kind, 2 * s + t, buf.at[m, t], part(out, chip, t), m, lax.rem(core + t, 2)).wait_send()
                    remote(kind, 2 * s + t, buf.at[m, t], part(out, h, t), m, core).wait_recv()
        for kind, buf, out in ((DK, k_all, dk_out), (DV, v_all, dv_out)):
            if s == 0:
                local(kind, 0, buf.at[0, chip], out.at[chip]).wait()
            else:
                remote(kind, s, buf.at[0, m], out.at[chip], m, core).wait_send()
                remote(kind, s, buf.at[0, m], out.at[h], m, core).wait_recv()


def solution(mesh):
    n_chip = mesh.shape['ctx'] // 2
    seq_spec = P('dp', 'ctx', None, None)

    def local_attn(q_loc, k_loc, v_loc, do_loc):
        _, chunk, q_heads, dim = q_loc.shape
        kv_heads = k_loc.shape[2]
        n_grp = q_heads // kv_heads
        blk_len = chunk // 2
        rows = n_grp * blk_len
        bf16, f32 = jnp.bfloat16, jnp.float32

        def split_q(x):
            return jnp.transpose(x.reshape(chunk, kv_heads, n_grp, dim), (1, 2, 0, 3))

        def split_kv(x):
            return jnp.transpose(x.reshape(chunk, kv_heads, dim), (1, 0, 2))

        q_shape, kv_shape = (n_chip, 2, n_grp, blk_len, dim), (n_chip, chunk, dim)
        q_type, kv_type = jax.ShapeDtypeStruct((n_chip, n_grp, chunk, dim), bf16), jax.ShapeDtypeStruct(kv_shape, bf16)
        o_all, dq_all, dk_all, dv_all = pl.pallas_call(
            attn_kernel,
            out_shape=(q_type, q_type, kv_type, kv_type),
            in_specs=[pl.BlockSpec(memory_space=pl.ANY)] * 4,
            out_specs=[pl.BlockSpec(memory_space=pl.ANY)] * 4,
            scratch_shapes=[
                pltpu.VMEM(q_shape, bf16),
                pltpu.VMEM(q_shape, bf16),
                pltpu.VMEM((2,) + kv_shape, bf16),
                pltpu.VMEM((2,) + kv_shape, bf16),
                pltpu.VMEM((2, n_chip, dim, chunk), bf16),
                pltpu.VMEM((2,) + kv_shape, f32),
                pltpu.VMEM((2,) + kv_shape, f32),
                pltpu.VMEM(q_shape, bf16),
                pltpu.VMEM(q_shape, bf16),
                pltpu.VMEM(kv_shape, f32),
                pltpu.VMEM(kv_shape, f32),
                pltpu.VMEM((dim, rows), f32),
                pltpu.VMEM((blk_len, rows), f32),
                pltpu.VMEM((1, rows), f32),
                pltpu.VMEM((1, rows), f32),
                pltpu.VMEM((2 * n_chip, 8, rows), f32),
                pltpu.VMEM((2, dim, rows), f32),
                pltpu.SemaphoreType.DMA((12, 8)),
                pltpu.SemaphoreType.DMA((12, 8)),
            ],
            compiler_params=pltpu.CompilerParams(vmem_limit_bytes=67043328, collective_id=0, has_side_effects=True),
        )(split_q(q_loc), split_q(do_loc), split_kv(k_loc), split_kv(v_loc))

        def join_q(x):
            return jnp.transpose(x, (2, 0, 1, 3)).reshape(q_loc.shape)

        def join_kv(x):
            return jnp.transpose(x, (1, 0, 2)).reshape(k_loc.shape)

        return join_q(o_all), join_q(dq_all), join_kv(dk_all), join_kv(dv_all)

    return jax.shard_map(local_attn, mesh=mesh, in_specs=(seq_spec,) * 4, out_specs=(seq_spec,) * 4, check_vma=False)
```
